16 devices in a mesh: data: 2 (over y, z), expert: 8 (over x, core).
Axes of the slice: x: 4, y: 2, z: 1, core: 2. Of those that a mesh axis runs over, the one named last changes fastest.
The devices are a block of a 4x4x8 slice.
Arguments:
- x_tok: bfloat16 [32768, 2048], P(('data', 'expert')), parts along dimension 0
- topk_idx: int32 [32768, 2], P(('data', 'expert')), parts along dimension 0
- topk_w: float32 [32768, 2], P(('data', 'expert')), parts along dimension 0
- w_up: bfloat16 [8, 2048, 5632], P('expert')
- w_down: bfloat16 [8, 5632, 2048], P('expert')
Outputs:
- output: bfloat16 [32768, 2048], P(('data', 'expert')), parts along dimension 0
There are 2 independent parts. The reference program is written for one: setup_inputs(seed, part) draws one part's arguments, and reference() takes and returns one part's arrays. A program takes and returns all parts, laid end to end along the dimension named above; an argument that names none is the same for every part.
All inputs are finite; a program needn't handle non-finite values.
Results may differ from the reference program's by a relative error of at most 0.0013.
Values are sent between devices in bfloat16 or wider.
A program may use at most 768 MiB of HBM per device.

```python
import jax
import jax.numpy as jnp
from jax import lax

D_MODEL = 2048
D_FF = 5632
EXPERTS = 8
TOP_K = 2
TOK_DEV = 2048
GROUP_SIZE = 8
HOT_MUL = min(4, EXPERTS // TOP_K)
SLOT_CAP = HOT_MUL * TOK_DEV * TOP_K // EXPERTS
NUM_HOT = max(1, EXPERTS // 32)
TOKENS = GROUP_SIZE * TOK_DEV


def draw_routing(key):
    hot_key, dev_key = jax.random.split(key)
    exp_perm = jax.random.permutation(hot_key, EXPERTS)
    n_cold = EXPERTS - NUM_HOT
    cold_total = TOK_DEV * TOP_K - NUM_HOT * SLOT_CAP
    base_count = cold_total // n_cold
    extra_count = cold_total - base_count * n_cold

    def one_device(dev_seed):
        shift_key, order_key, perm_key = jax.random.split(dev_seed, 3)
        shifts = jax.random.randint(shift_key, (n_cold // 2,), 0, base_count // 2 + 1)
        count_shift = jnp.concatenate([jnp.stack([shifts, -shifts], axis=1).reshape(-1), jnp.zeros((n_cold % 2,), jnp.int32)])
        cold_counts = base_count + (jnp.arange(n_cold) < extra_count).astype(jnp.int32) + count_shift
        counts = jnp.concatenate([jnp.full((NUM_HOT,), SLOT_CAP, jnp.int32), cold_counts])
        visit_order = jax.random.permutation(order_key, EXPERTS)
        run_ends = jnp.cumsum(counts[visit_order])
        run_index = jnp.searchsorted(run_ends, jnp.arange(TOK_DEV * TOP_K), side='right')
        pair_seq = exp_perm[visit_order][run_index]
        choice = pair_seq.reshape(TOP_K, TOK_DEV).T
        return choice[jax.random.permutation(perm_key, TOK_DEV)]

    dev_keys = jax.random.split(dev_key, GROUP_SIZE)
    return jax.vmap(one_device)(dev_keys).reshape(TOKENS, TOP_K).astype(jnp.int32)


def setup_inputs(seed: int = 0, part: int = 0) -> dict:
    part_key = jax.random.fold_in(jax.random.key(seed), part)
    route_key, gate_key, tok_key = jax.random.split(part_key, 3)
    up_key, down_key = jax.random.split(jax.random.key(seed + 1))
    x_tok = jax.random.normal(tok_key, (TOKENS, D_MODEL), jnp.float32).astype(jnp.bfloat16)
    topk_idx = draw_routing(route_key)
    topk_w = jax.random.uniform(gate_key, (TOKENS, TOP_K), jnp.float32, 0.1, 1.0)
    w_up = (jax.random.normal(up_key, (EXPERTS, D_MODEL, D_FF), jnp.float32) * D_MODEL ** -0.5).astype(jnp.bfloat16)
    w_down = (jax.random.normal(down_key, (EXPERTS, D_FF, D_MODEL), jnp.float32) * D_FF ** -0.5).astype(jnp.bfloat16)
    return {'x_tok': x_tok, 'topk_idx': topk_idx, 'topk_w': topk_w, 'w_up': w_up, 'w_down': w_down}


def reference(x_tok, topk_idx, topk_w, w_up, w_down):
    pair_exp = topk_idx.reshape(-1)
    n_pairs = TOKENS * TOP_K
    group_cap = GROUP_SIZE * SLOT_CAP
    sort_order = jnp.argsort(pair_exp, stable=True)
    pair_rank = jnp.argsort(sort_order, stable=True)
    counts = jnp.bincount(pair_exp, length=EXPERTS)
    starts = jnp.cumsum(counts) - counts
    slot_src = jnp.minimum(starts[:, None] + jnp.arange(group_cap)[None, :], n_pairs - 1)
    slot_tok = sort_order[slot_src] // TOP_K

    def expert_rows(operands):
        tok_ids, up_mat, down_mat = operands
        tok_rows = x_tok[tok_ids]
        hidden = jnp.dot(tok_rows, up_mat, preferred_element_type=jnp.float32)
        hidden = jax.nn.gelu(hidden, approximate=True).astype(jnp.bfloat16)
        return jnp.dot(hidden, down_mat, preferred_element_type=jnp.float32).astype(jnp.bfloat16)

    slot_out = lax.map(expert_rows, (slot_tok, w_up, w_down)).reshape(EXPERTS * group_cap, D_MODEL)
    pair_slot = pair_exp * group_cap + pair_rank - starts[pair_exp]
    pair_out = slot_out[pair_slot].reshape(TOKENS, TOP_K, D_MODEL)
    y_tok = jnp.sum(topk_w[:, :, None] * pair_out.astype(jnp.float32), axis=1)
    return y_tok.astype(jnp.bfloat16)
```

```python
import jax
import jax.numpy as jnp
from jax import lax
from jax.sharding import PartitionSpec as P

SLOTS = 448


def gelu(v):
    return jax.nn.gelu(v, approximate=True)


def ffn_in(rows, up):
    hidden = jnp.dot(rows, up, preferred_element_type=jnp.float32)
    return gelu(hidden).astype(jnp.bfloat16)


def ffn_out(hidden, down):
    out = jnp.dot(hidden, down, preferred_element_type=jnp.float32)
    return lax.reduce_precision(out, 8, 7).astype(jnp.bfloat16)


def solution(mesh):
    group = mesh.shape['expert']
    axes = tuple(mesh.axis_names)

    def local_moe(x, idx, gate, up, down):
        n_tok, d_model = x.shape
        up, down = up[0], down[0]
        n_exp = group
        me = lax.axis_index('expert')
        experts = jnp.arange(n_exp, dtype=jnp.int32)

        counts = jnp.sum((idx[:, :, None] == experts).astype(jnp.int32), axis=(0, 1))
        hot = jnp.argmax(counts).astype(jnp.int32)
        first_hot = idx[:, 0] == hot
        cold = jnp.where(first_hot, idx[:, 1], idx[:, 0])
        gate_hot = jnp.where(first_hot, gate[:, 0], gate[:, 1])[:, None]
        gate_cold = jnp.where(first_hot, gate[:, 1], gate[:, 0])[:, None]

        def share(w):
            return lax.psum_scatter(jnp.where(me == hot, w, jnp.zeros_like(w)), 'expert', scatter_dimension=0, tiled=True)

        up_share = share(up)

        cold_counts = jnp.where(experts == hot, 0, counts)
        mine = (cold[:, None] == experts).astype(jnp.int32).reshape(n_tok // 128, 128, n_exp)
        lower = jnp.tril(jnp.ones((128, 128), jnp.float32), -1)
        within = jnp.einsum('ij,bje->bie', lower, mine.astype(jnp.float32)).astype(jnp.int32)
        block_sum = jnp.sum(mine, axis=1)
        before = jnp.cumsum(block_sum, axis=0) - block_sum
        rank = jnp.sum(mine * (before[:, None, :] + within), axis=-1).reshape(-1)
        rounds = lax.pmax((jnp.max(cold_counts) + SLOTS - 1) // SLOTS, axes)

        def outward(r):
            here = rank - r * SLOTS
            slot = jnp.where((here >= 0) & (here < SLOTS), cold * SLOTS + here, -1)
            hit = slot[None, :] == jnp.arange(n_exp * SLOTS, dtype=jnp.int32)[:, None]
            slot_tok = jnp.sum(jnp.where(hit, jnp.arange(n_tok, dtype=jnp.int32)[None, :], 0), axis=1)
            send = x.at[slot_tok].get(mode='promise_in_bounds').reshape(n_exp, SLOTS, d_model)
            return lax.all_to_all(send, 'expert', 0, 0, tiled=True).reshape(n_exp * SLOTS, d_model)

        def homeward(r, hidden):
            out = ffn_out(hidden, down).reshape(n_exp, SLOTS, d_model)
            return lax.all_to_all(out, 'expert', 0, 0, tiled=True).reshape(n_exp * SLOTS, d_model)

        def pick(r, back):
            here = jnp.clip(rank - r * SLOTS, 0, SLOTS - 1)
            return back.at[cold * SLOTS + here].get(mode='promise_in_bounds')

        def combine(hot_out, cold_row):
            return (gate_hot * hot_out.astype(jnp.float32) + gate_cold * cold_row.astype(jnp.float32)).astype(jnp.bfloat16)

        recv, late_down = lax.optimization_barrier((outward(0), down))
        down_share = share(late_down)
        hidden, down_share = lax.optimization_barrier((ffn_in(recv, up), down_share))
        back = homeward(0, hidden)
        hot_up = lax.all_gather(up_share, 'expert', axis=0, tiled=True)
        hot_down = lax.all_gather(down_share, 'expert', axis=0, tiled=True)
        hot_hidden, back = lax.optimization_barrier((ffn_in(x, hot_up), back))
        cold_row = pick(0, back)
        hot_out = ffn_out(hot_hidden, hot_down)
        y = combine(hot_out, cold_row)

        def more(state):
            r, y = state
            new = combine(hot_out, pick(r, homeward(r, ffn_in(outward(r), up))))
            return r + 1, jnp.where((rank // SLOTS == r)[:, None], new, y)

        return lax.while_loop(lambda state: state[0] < rounds, more, (jnp.int32(1), y))[1]

    tok_spec = P(('data', 'expert'), None)
    w_spec = P('expert', None, None)
    return jax.shard_map(local_moe, mesh=mesh, in_specs=(tok_spec, tok_spec, tok_spec, w_spec, w_spec), out_specs=tok_spec, check_vma=False)
```

```python
import functools

import jax
import jax.numpy as jnp
from jax import lax
from jax.experimental import pallas as pl
from jax.experimental.pallas import tpu as pltpu
from jax.sharding import PartitionSpec as P

SLOTS = 448
SUB = 256
SUBS = 7
FF_STEP = 512
RING = 64
MESH = pl.DeviceIdType.MESH


class Way:
    def __init__(self, pieces, lag, group):
        self.pieces, self.lag = pieces, lag
        self.slots = pieces + (group - 2) * lag

    def bind(self, owner, weights, landed, both, out, own_sem, got_sem, send_sem, recv_sem, target):
        self.owner, self.weights, self.landed, self.both, self.out = owner, weights, landed, both, out
        self.own_sem, self.got_sem, self.send_sem, self.recv_sem, self.target = own_sem, got_sem, send_sem, recv_sem, target

    def remote(self, t):
        return pltpu.make_async_remote_copy(
            src_ref=self.out.at[t % 3], dst_ref=self.landed.at[t], send_sem=self.send_sem.at[t % 3],
            recv_sem=self.recv_sem.at[t % RING], device_id={'expert': self.target}, device_id_type=MESH)

    def own(self, t):
        return pltpu.make_async_copy(self.weights.at[t], self.both.at[t % 2, 1], self.own_sem.at[t % 2])

    def got(self, t):
        return pltpu.make_async_copy(self.landed.at[t - self.lag], self.both.at[t % 2, 0], self.got_sem.at[t % 2])

    def load(self, t):
        @pl.when(t < self.pieces)
        def _():
            self.own(t).start()

        @pl.when(t >= self.lag)
        def _():
            self.remote(t - self.lag).wait_recv()
            self.got(t).start()

    def choose(self, t):
        @pl.when(t < self.pieces)
        def _():
            self.own(t).wait()

        @pl.when(t >= self.lag)
        def _():
            self.got(t).wait()

        @pl.when(t >= 3)
        def _():
            self.remote(t - 3).wait_send()

        which = jnp.where(t < self.lag, 1, jnp.where(t < self.pieces, self.owner[0], 0))
        self.out[t % 3] = self.both[t % 2, which]

    def event(self, t):
        @pl.when((t >= 1) & (t <= self.slots))
        def _():
            self.remote(t - 1).start()

        @pl.when(t < self.slots)
        def _():
            self.choose(t)

        @pl.when(t + 1 < self.slots)
        def _():
            self.load(t + 1)

    def finish(self):
        for t in range(self.slots - 3, self.slots):
            self.remote(t).wait_send()
        for t in range(self.slots - self.lag, self.slots):
            self.remote(t).wait_recv()


def ring_ffn_kernel(group, up_way, down_way, owner, x_hbm, up_hbm, down_hbm, up_pieces, down_pieces,
                    o_hbm, up_landed, down_landed,
                    x_buf, acc, up_buf, down_buf, o_buf, x_sem, w_sem, o_sem,
                    up_both, up_out, up_own_sem, up_got_sem, up_send_sem, up_recv_sem,
                    down_both, down_out, down_own_sem, down_got_sem, down_send_sem, down_recv_sem):
    me = lax.axis_index('expert')
    right, left = lax.rem(me + 1, group), lax.rem(me + group - 1, group)
    barrier = pltpu.get_barrier_semaphore()
    for other in (left, right):
        pl.semaphore_signal(barrier, inc=1, device_id={'expert': other}, device_id_type=MESH)
    pl.semaphore_wait(barrier, 2)
    up_way.bind(owner, up_pieces, up_landed, up_both, up_out, up_own_sem, up_got_sem, up_send_sem, up_recv_sem, right)
    down_way.bind(owner, down_pieces, down_landed, down_both, down_out, down_own_sem, down_got_sem, down_send_sem, down_recv_sem, left)

    big = SUB * SUBS
    supers = x_hbm.shape[0] // big
    n_ff = up_hbm.shape[1] // FF_STEP
    steps = supers * n_ff

    def x_copy(p):
        return pltpu.make_async_copy(x_hbm.at[pl.ds(pl.multiple_of(p * big, big), big)], x_buf.at[p % 2], x_sem.at[p % 2])

    def w_copies(s):
        cols = pl.ds(pl.multiple_of((s % n_ff) * FF_STEP, FF_STEP), FF_STEP)
        return (pltpu.make_async_copy(up_hbm.at[:, cols], up_buf.at[s % 2], w_sem.at[0, s % 2]),
                pltpu.make_async_copy(down_hbm.at[cols], down_buf.at[s % 2], w_sem.at[1, s % 2]))

    def o_copy(i):
        return pltpu.make_async_copy(o_buf.at[i % 2], o_hbm.at[pl.ds(pl.multiple_of(i * SUB, SUB), SUB)], o_sem.at[i % 2])

    def compute(e):
        s, sub = e // SUBS, e % SUBS
        p, f = s // n_ff, s % n_ff

        @pl.when((sub == 0) & (f == 0))
        def _():
            x_copy(p).wait()

            @pl.when(p + 1 < supers)
            def _():
                x_copy(p + 1).start()

        @pl.when(sub == 0)
        def _():
            for c in w_copies(s):
                c.wait()

            @pl.when(s + 1 < steps)
            def _():
                for c in w_copies(s + 1):
                    c.start()

        rows = pl.ds(pl.multiple_of(sub * SUB, SUB), SUB)
        h = jnp.dot(x_buf[p % 2, rows, :], up_buf[s % 2], preferred_element_type=jnp.float32)
        h = gelu(h).astype(jnp.bfloat16)
        part = jnp.dot(h, down_buf[s % 2], preferred_element_type=jnp.float32)

        @pl.when(f == 0)
        def _():
            acc[rows, :] = part

        @pl.when((f > 0) & (f < n_ff - 1))
        def _():
            acc[rows, :] += part

        @pl.when(f == n_ff - 1)
        def _():
            i = p * SUBS + sub

            @pl.when(i >= 2)
            def _():
                o_copy(i - 2).wait()
            o_buf[i % 2] = (acc[rows, :] + part).astype(jnp.bfloat16)
            o_copy(i).start()

    x_copy(0).start()
    for c in w_copies(0):
        c.start()
    up_way.load(0)
    down_way.load(0)

    def body(e, carry):
        @pl.when(e <= up_way.slots)
        def _():
            up_way.event(e)

        b = (e // 4) * 3 + e % 4

        @pl.when((e % 4 != 3) & (b <= down_way.slots))
        def _():
            down_way.event(b)

        @pl.when(e < steps * SUBS)
        def _():
            compute(e)
        return carry

    n_events = max(steps * SUBS, up_way.slots + 1, (down_way.slots // 3 + 1) * 4)
    lax.fori_loop(0, n_events, body, 0)
    up_way.finish()
    down_way.finish()
    n_out = supers * SUBS
    o_copy(n_out - 2).wait()
    o_copy(n_out - 1).wait()


def ring_ffn(group, owner, x, up, down):
    n_rows, d_model = x.shape
    d_ff = up.shape[1]
    up_rows, down_rows = 16, 64
    up_way, down_way = Way(d_model // up_rows, 5, group), Way(d_ff // down_rows, 4, group)
    up_pieces = up.reshape(d_model // up_rows, up_rows, d_ff)
    down_pieces = down.reshape(d_ff // down_rows, down_rows, d_model)
    hbm = pl.BlockSpec(memory_space=pl.ANY)
    big = SUB * SUBS
    dma = pltpu.SemaphoreType.DMA

    def ring_scratch(rows, cols):
        return [pltpu.VMEM((2, 2, rows, cols), jnp.bfloat16), pltpu.VMEM((3, rows, cols), jnp.bfloat16),
                dma((2,)), dma((2,)), dma((3,)), dma((RING,))]

    out, up_landed, down_landed = pl.pallas_call(
        functools.partial(ring_ffn_kernel, group, up_way, down_way),
        out_shape=(jax.ShapeDtypeStruct((n_rows, d_model), jnp.bfloat16),
                   jax.ShapeDtypeStruct((up_way.slots, up_rows, d_ff), jnp.bfloat16),
                   jax.ShapeDtypeStruct((down_way.slots, down_rows, d_model), jnp.bfloat16)),
        in_specs=[pl.BlockSpec(memory_space=pltpu.SMEM), hbm, hbm, hbm, hbm, hbm],
        out_specs=(hbm, hbm, hbm),
        scratch_shapes=[
            pltpu.VMEM((2, big, d_model), jnp.bfloat16),
            pltpu.VMEM((big, d_model), jnp.float32),
            pltpu.VMEM((2, d_model, FF_STEP), jnp.bfloat16),
            pltpu.VMEM((2, FF_STEP, d_model), jnp.bfloat16),
            pltpu.VMEM((2, SUB, d_model), jnp.bfloat16),
            dma((2,)), dma((2, 2)), dma((2,)),
        ] + ring_scratch(up_rows, d_ff) + ring_scratch(down_rows, d_model),
        compiler_params=pltpu.CompilerParams(collective_id=0, has_side_effects=True, vmem_limit_bytes=60 * 1024 * 1024),
        cost_estimate=pl.CostEstimate(flops=4 * n_rows * d_model * d_ff, bytes_accessed=8 * d_model * d_ff, transcendentals=0),
        name="ring_ffn",
    )(owner.reshape(1), x, up, down, up_pieces, down_pieces)

    def whole(landed, way, rows, distance, own):
        first = jnp.maximum(distance - 1, 0) * way.lag * rows
        flat = landed.reshape(-1, landed.shape[-1])
        return jnp.where(owner == 1, own, lax.dynamic_slice_in_dim(flat, first, own.shape[0], 0))

    return out, lambda hot, me: (
        whole(up_landed, up_way, up_rows, (me - hot) % group, up),
        whole(down_landed, down_way, down_rows, (hot - me) % group, down))


def gelu(v):
    return jax.nn.gelu(v, approximate=True)


def ffn_in(rows, up):
    hidden = jnp.dot(rows, up, preferred_element_type=jnp.float32)
    return gelu(hidden).astype(jnp.bfloat16)


def ffn_out(hidden, down):
    out = jnp.dot(hidden, down, preferred_element_type=jnp.float32)
    return lax.reduce_precision(out, 8, 7).astype(jnp.bfloat16)


def solution(mesh):
    group = mesh.shape['expert']
    axes = tuple(mesh.axis_names)

    def local_moe(x, idx, gate, up, down):
        n_tok, d_model = x.shape
        up, down = up[0], down[0]
        n_exp = group
        me = lax.axis_index('expert')
        experts = jnp.arange(n_exp, dtype=jnp.int32)

        counts = jnp.sum((idx[:, :, None] == experts).astype(jnp.int32), axis=(0, 1))
        hot = jnp.argmax(counts).astype(jnp.int32)
        first_hot = idx[:, 0] == hot
        cold = jnp.where(first_hot, idx[:, 1], idx[:, 0])
        gate_hot = jnp.where(first_hot, gate[:, 0], gate[:, 1])[:, None]
        gate_cold = jnp.where(first_hot, gate[:, 1], gate[:, 0])[:, None]

        cold_counts = jnp.where(experts == hot, 0, counts)
        rounds = lax.pmax((jnp.max(cold_counts) + SLOTS - 1) // SLOTS, axes)
        cold, rounds = lax.optimization_barrier((cold, rounds))
        mine = (cold[:, None] == experts).astype(jnp.int32).reshape(n_tok // 128, 128, n_exp)
        lower = jnp.tril(jnp.ones((128, 128), jnp.float32), -1)
        within = jnp.einsum('ij,bje->bie', lower, mine.astype(jnp.float32)).astype(jnp.int32)
        block_sum = jnp.sum(mine, axis=1)
        before = jnp.cumsum(block_sum, axis=0) - block_sum
        rank = jnp.sum(mine * (before[:, None, :] + within), axis=-1).reshape(-1)
        def outward(r):
            here = rank - r * SLOTS
            slot = jnp.where((here >= 0) & (here < SLOTS), cold * SLOTS + here, -1)
            hit = slot[None, :] == jnp.arange(n_exp * SLOTS, dtype=jnp.int32)[:, None]
            slot_tok = jnp.sum(jnp.where(hit, jnp.arange(n_tok, dtype=jnp.int32)[None, :], 0), axis=1)
            send = x.at[slot_tok].get(mode='promise_in_bounds').reshape(n_exp, SLOTS, d_model)
            return lax.all_to_all(send, 'expert', 0, 0, tiled=True).reshape(n_exp * SLOTS, d_model)

        def homeward(r, hidden):
            out = ffn_out(hidden, down).reshape(n_exp, SLOTS, d_model)
            return lax.all_to_all(out, 'expert', 0, 0, tiled=True).reshape(n_exp * SLOTS, d_model)

        def pick(r, back):
            here = jnp.clip(rank - r * SLOTS, 0, SLOTS - 1)
            return back.at[cold * SLOTS + here].get(mode='promise_in_bounds')

        def combine(hot_out, cold_row):
            return (gate_hot * hot_out.astype(jnp.float32) + gate_cold * cold_row.astype(jnp.float32)).astype(jnp.bfloat16)

        owner = (me == hot).astype(jnp.int32)
        cold_out, gather_hot = ring_ffn(group, owner, outward(0), up, down)
        back = lax.all_to_all(cold_out.reshape(n_exp, SLOTS, d_model), 'expert', 0, 0, tiled=True).reshape(n_exp * SLOTS, d_model)
        hot_up, hot_down = gather_hot(hot, me)
        hot_hidden = ffn_in(x, hot_up)
        hot_out = ffn_out(hot_hidden, hot_down)
        hot_out, back = lax.optimization_barrier((hot_out, back))
        cold_row = pick(0, back)
        y = combine(hot_out, cold_row)

        def more(state):
            r, y = state
            new = combine(hot_out, pick(r, homeward(r, ffn_in(outward(r), up))))
            return r + 1, jnp.where((rank // SLOTS == r)[:, None], new, y)

        return lax.while_loop(lambda state: state[0] < rounds, more, (jnp.int32(1), y))[1]

    tok_spec = P(('data', 'expert'), None)
    w_spec = P('expert', None, None)
    return jax.shard_map(local_moe, mesh=mesh, in_specs=(tok_spec, tok_spec, tok_spec, w_spec, w_spec), out_specs=tok_spec, check_vma=False)
```

```python
import functools

import jax
import jax.numpy as jnp
from jax import lax
from jax.experimental import pallas as pl
from jax.experimental.pallas import tpu as pltpu
from jax.sharding import PartitionSpec as P

SLOTS = 440
SUB = 352
SUBS = 5
FF_STEP = 1408
FF_CUTS = 0, 768, 1408
OUT_PART = 1024
RING = 64
PIECE_ROWS = 16, 64
LAGS = (5, 3), (4, 3)
UP_TICKS = 25, 18
TICKS = 4
MESH = pl.DeviceIdType.MESH


class Way:
    def __init__(self, pieces, lags, near, group):
        self.pieces, self.lags, self.near = pieces, lags, near
        self.slots = pieces + (group - 2) // 2 * sum(lags)

    def shift(self, hot, distance):
        relays = jnp.maximum(distance - 1, 0)
        near = (relays + (hot % 2 != self.near)) // 2
        return near * self.lags[1] + (relays - near) * self.lags[0]

    def bind(self, me, owner, weights, landed, both, out, own_sem, got_sem, send_sem, recv_sem, target):
        self.lag = jnp.where(me % 2 == self.near, self.lags[1], self.lags[0])
        self.owner, self.weights, self.landed, self.both, self.out = owner, weights, landed, both, out
        self.own_sem, self.got_sem, self.send_sem, self.recv_sem, self.target = own_sem, got_sem, send_sem, recv_sem, target

    def remote(self, t):
        return pltpu.make_async_remote_copy(
            src_ref=self.out.at[t % 3], dst_ref=self.landed.at[t], send_sem=self.send_sem.at[t % 3],
            recv_sem=self.recv_sem.at[t % RING], device_id={'expert': self.target}, device_id_type=MESH)

    def own(self, t):
        return pltpu.make_async_copy(self.weights.at[t], self.both.at[t % 2, 1], self.own_sem.at[t % 2])

    def got(self, t):
        return pltpu.make_async_copy(self.landed.at[t - self.lag], self.both.at[t % 2, 0], self.got_sem.at[t % 2])

    def load(self, t):
        @pl.when(t < self.pieces)
        def _():
            self.own(t).start()

        @pl.when(t >= self.lag)
        def _():
            self.remote(t - self.lag).wait_recv()
            self.got(t).start()

    def choose(self, t):
        @pl.when(t < self.pieces)
        def _():
            self.own(t).wait()

        @pl.when(t >= self.lag)
        def _():
            self.got(t).wait()

        @pl.when(t >= 3)
        def _():
            self.remote(t - 3).wait_send()

        which = jnp.where(t < self.lag, 1, jnp.where(t < self.pieces, self.owner[0], 0))
        self.out[t % 3] = self.both[t % 2, which]

    def event(self, t):
        @pl.when((t >= 1) & (t <= self.slots))
        def _():
            self.remote(t - 1).start()

        @pl.when(t < self.slots)
        def _():
            self.choose(t)

        @pl.when(t + 1 < self.slots)
        def _():
            self.load(t + 1)

    def finish(self):
        for t in range(self.slots - 3, self.slots):
            self.remote(t).wait_send()
        for t in range(self.slots - self.lags[0], self.slots):
            @pl.when(t >= self.slots - self.lag)
            def _():
                self.remote(t).wait_recv()


def ring_ffn_kernel(group, up_way, down_way, owner, x_hbm, up_hbm, down_hbm, up_pieces, down_pieces,
                    o_hbm, up_landed, down_landed,
                    x_buf, acc, up_buf, down_buf, h_buf, o_buf, x_sem, w_sem, o_sem,
                    up_both, up_out, up_own_sem, up_got_sem, up_send_sem, up_recv_sem,
                    down_both, down_out, down_own_sem, down_got_sem, down_send_sem, down_recv_sem):
    me = lax.axis_index('expert')
    right, left = lax.rem(me + 1, group), lax.rem(me + group - 1, group)
    barrier = pltpu.get_barrier_semaphore()
    for other in (left, right):
        pl.semaphore_signal(barrier, inc=1, device_id={'expert': other}, device_id_type=MESH)
    pl.semaphore_wait(barrier, 2)
    up_way.bind(me, owner, up_pieces, up_landed, up_both, up_out, up_own_sem, up_got_sem, up_send_sem, up_recv_sem, right)
    down_way.bind(me, owner, down_pieces, down_landed, down_both, down_out, down_own_sem, down_got_sem, down_send_sem, down_recv_sem, left)

    big = SUB * SUBS
    supers = x_hbm.shape[0] // big
    n_ff = up_hbm.shape[1] // FF_STEP
    steps = supers * n_ff

    def x_copy(p):
        return pltpu.make_async_copy(x_hbm.at[pl.ds(pl.multiple_of(p * big, big), big)], x_buf.at[p % 2], x_sem.at[p % 2])

    def w_copies(s):
        cols = pl.ds(pl.multiple_of((s % n_ff) * FF_STEP, FF_STEP), FF_STEP)
        return (pltpu.make_async_copy(up_hbm.at[:, cols], up_buf.at[s % 2], w_sem.at[0, s % 2]),
                pltpu.make_async_copy(down_hbm.at[cols], down_buf.at[s % 2], w_sem.at[1, s % 2]))

    def o_copy(i):
        return pltpu.make_async_copy(o_buf.at[i % 2], o_hbm.at[pl.ds(pl.multiple_of(i * SUB, SUB), SUB)], o_sem.at[i % 2])

    def place(e):
        s, sub = e // SUBS, e % SUBS
        return s, sub, s // n_ff, s % n_ff, pl.ds(pl.multiple_of(sub * SUB, SUB), SUB)

    def compute_start(e):
        s, sub, p, f, rows = place(e)

        @pl.when((sub == 0) & (f == 0))
        def _():
            x_copy(p).wait()

            @pl.when(p + 1 < supers)
            def _():
                x_copy(p + 1).start()

        @pl.when(sub == 0)
        def _():
            for c in w_copies(s):
                c.wait()

            @pl.when(s + 1 < steps)
            def _():
                for c in w_copies(s + 1):
                    c.start()

    def compute_in(e, lo, hi):
        s, sub, p, f, rows = place(e)
        h = jnp.dot(x_buf[p % 2, rows, :], up_buf[s % 2, :, lo:hi], preferred_element_type=jnp.float32)
        h_buf[:, lo:hi] = gelu(h).astype(jnp.bfloat16)

    def compute_out(e, lo, hi):
        s, sub, p, f, rows = place(e)
        part = jnp.dot(h_buf[...], down_buf[s % 2, :, lo:hi], preferred_element_type=jnp.float32)

        @pl.when(f == 0)
        def _():
            acc[rows, lo:hi] = part

        @pl.when((f > 0) & (f < n_ff - 1))
        def _():
            acc[rows, lo:hi] += part

        @pl.when(f == n_ff - 1)
        def _():
            i = p * SUBS + sub
            if lo == 0:
                @pl.when(i >= 2)
                def _():
                    o_copy(i - 2).wait()
            o_buf[i % 2, :, lo:hi] = (acc[rows, lo:hi] + part).astype(jnp.bfloat16)
            if hi == o_buf.shape[2]:
                o_copy(i).start()

    x_copy(0).start()
    for c in w_copies(0):
        c.start()
    up_way.load(0)
    down_way.load(0)

    more, less = UP_TICKS

    def tick(n):
        @pl.when(n <= up_way.slots)
        def _():
            up_way.event(n)

        b = n * less // more

        @pl.when(((n + 1) * less // more > b) & (b <= down_way.slots))
        def _():
            down_way.event(b)

    d_model = o_buf.shape[2]
    work = [functools.partial(compute_in, lo=lo, hi=hi) for lo, hi in zip(FF_CUTS[:-1], FF_CUTS[1:])]
    work += [functools.partial(compute_out, lo=lo, hi=lo + OUT_PART) for lo in range(0, d_model, OUT_PART)]

    def body(e, carry):
        live = e < steps * SUBS

        @pl.when(live)
        def _():
            compute_start(e)
        for i, part in enumerate(work):
            if i < TICKS:
                tick(e * TICKS + i)

            @pl.when(live)
            def _():
                part(e)
        return carry

    n_ticks = max(up_way.slots + 1, ((down_way.slots + 1) * more + less - 1) // less + 1)
    lax.fori_loop(0, max(steps * SUBS, -(-n_ticks // TICKS)), body, 0)
    up_way.finish()
    down_way.finish()
    n_out = supers * SUBS
    o_copy(n_out - 2).wait()
    o_copy(n_out - 1).wait()


def ring_ffn(group, owner, x, up, down):
    n_rows, d_model = x.shape
    d_ff = up.shape[1]
    up_rows, down_rows = PIECE_ROWS
    up_way, down_way = Way(d_model // up_rows, LAGS[0], 1, group), Way(d_ff // down_rows, LAGS[1], 0, group)
    up_pieces = up.reshape(d_model // up_rows, up_rows, d_ff)
    down_pieces = down.reshape(d_ff // down_rows, down_rows, d_model)
    hbm = pl.BlockSpec(memory_space=pl.ANY)
    big = SUB * SUBS
    dma = pltpu.SemaphoreType.DMA

    def ring_scratch(rows, cols):
        return [pltpu.VMEM((2, 2, rows, cols), jnp.bfloat16), pltpu.VMEM((3, rows, cols), jnp.bfloat16),
                dma((2,)), dma((2,)), dma((3,)), dma((RING,))]

    out, up_landed, down_landed = pl.pallas_call(
        functools.partial(ring_ffn_kernel, group, up_way, down_way),
        out_shape=(jax.ShapeDtypeStruct((n_rows, d_model), jnp.bfloat16),
                   jax.ShapeDtypeStruct((up_way.slots, up_rows, d_ff), jnp.bfloat16),
                   jax.ShapeDtypeStruct((down_way.slots, down_rows, d_model), jnp.bfloat16)),
        in_specs=[pl.BlockSpec(memory_space=pltpu.SMEM), hbm, hbm, hbm, hbm, hbm],
        out_specs=(hbm, hbm, hbm),
        scratch_shapes=[
            pltpu.VMEM((2, big, d_model), jnp.bfloat16),
            pltpu.VMEM((big, d_model), jnp.float32),
            pltpu.VMEM((2, d_model, FF_STEP), jnp.bfloat16),
            pltpu.VMEM((2, FF_STEP, d_model), jnp.bfloat16),
            pltpu.VMEM((SUB, FF_STEP), jnp.bfloat16),
            pltpu.VMEM((2, SUB, d_model), jnp.bfloat16),
            dma((2,)), dma((2, 2)), dma((2,)),
        ] + ring_scratch(up_rows, d_ff) + ring_scratch(down_rows, d_model),
        compiler_params=pltpu.CompilerParams(collective_id=0, has_side_effects=True, vmem_limit_bytes=62 * 1024 * 1024),
        cost_estimate=pl.CostEstimate(flops=4 * n_rows * d_model * d_ff, bytes_accessed=8 * d_model * d_ff, transcendentals=0),
        name="ring_ffn",
    )(owner.reshape(1), x, up, down, up_pieces, down_pieces)

    def whole(landed, way, rows, hot, distance, own):
        first = way.shift(hot, distance) * rows
        flat = landed.reshape(-1, landed.shape[-1])
        return jnp.where(owner == 1, own, lax.dynamic_slice_in_dim(flat, first, own.shape[0], 0))

    return out, lambda hot, me: (
        whole(up_landed, up_way, up_rows, hot, (me - hot) % group, up),
        whole(down_landed, down_way, down_rows, hot, (hot - me) % group, down))


def gelu(v):
    return jax.nn.gelu(v, approximate=True)


def ffn_in(rows, up):
    hidden = jnp.dot(rows, up, preferred_element_type=jnp.float32)
    return gelu(hidden).astype(jnp.bfloat16)


def ffn_out(hidden, down):
    out = jnp.dot(hidden, down, preferred_element_type=jnp.float32)
    return lax.reduce_precision(out, 8, 7).astype(jnp.bfloat16)


def solution(mesh):
    group = mesh.shape['expert']
    axes = tuple(mesh.axis_names)

    def local_moe(x, idx, gate, up, down):
        n_tok, d_model = x.shape
        up, down = up[0], down[0]
        n_exp = group
        me = lax.axis_index('expert')
        experts = jnp.arange(n_exp, dtype=jnp.int32)

        counts = jnp.sum((idx[:, :, None] == experts).astype(jnp.int32), axis=(0, 1))
        hot = jnp.argmax(counts).astype(jnp.int32)
        first_hot = idx[:, 0] == hot
        cold = jnp.where(first_hot, idx[:, 1], idx[:, 0])
        gate_hot = jnp.where(first_hot, gate[:, 0], gate[:, 1])[:, None]
        gate_cold = jnp.where(first_hot, gate[:, 1], gate[:, 0])[:, None]

        cold_counts = jnp.where(experts == hot, 0, counts)
        rounds = lax.pmax((jnp.max(cold_counts) + SLOTS - 1) // SLOTS, axes)
        mine = (cold[:, None] == experts).astype(jnp.int32).reshape(n_tok // 128, 128, n_exp)
        lower = jnp.tril(jnp.ones((128, 128), jnp.float32), -1)
        within = jnp.einsum('ij,bje->bie', lower, mine.astype(jnp.float32)).astype(jnp.int32)
        block_sum = jnp.sum(mine, axis=1)
        before = jnp.cumsum(block_sum, axis=0) - block_sum
        rank = jnp.sum(mine * (before[:, None, :] + within), axis=-1).reshape(-1)

        def outward(r):
            here = rank - r * SLOTS
            slot = jnp.where((here >= 0) & (here < SLOTS), cold * SLOTS + here, -1)
            hit = slot[None, :] == jnp.arange(n_exp * SLOTS, dtype=jnp.int32)[:, None]
            slot_tok = jnp.sum(jnp.where(hit, jnp.arange(n_tok, dtype=jnp.int32)[None, :], 0), axis=1)
            send = x.at[slot_tok].get(mode='promise_in_bounds').reshape(n_exp, SLOTS, d_model)
            return lax.all_to_all(send, 'expert', 0, 0, tiled=True).reshape(n_exp * SLOTS, d_model)

        def homeward(r, hidden):
            out = ffn_out(hidden, down).reshape(n_exp, SLOTS, d_model)
            return lax.all_to_all(out, 'expert', 0, 0, tiled=True).reshape(n_exp * SLOTS, d_model)

        def pick(r, back):
            here = jnp.clip(rank - r * SLOTS, 0, SLOTS - 1)
            return back.at[cold * SLOTS + here].get(mode='promise_in_bounds')

        def combine(hot_out, cold_row):
            return (gate_hot * hot_out.astype(jnp.float32) + gate_cold * cold_row.astype(jnp.float32)).astype(jnp.bfloat16)

        owner = (me == hot).astype(jnp.int32)
        recv, rounds = lax.optimization_barrier((outward(0), rounds))
        cold_out, gather_hot = ring_ffn(group, owner, recv, up, down)
        back = lax.all_to_all(cold_out.reshape(n_exp, SLOTS, d_model), 'expert', 0, 0, tiled=True).reshape(n_exp * SLOTS, d_model)
        hot_up, hot_down = gather_hot(hot, me)
        hot_hidden = ffn_in(x, hot_up)
        hot_out = ffn_out(hot_hidden, hot_down)
        hot_out, back = lax.optimization_barrier((hot_out, back))
        cold_row = pick(0, back)
        y = combine(hot_out, cold_row)

        def more(state):
            r, y = state
            new = combine(hot_out, pick(r, homeward(r, ffn_in(outward(r), up))))
            return r + 1, jnp.where((rank // SLOTS == r)[:, None], new, y)

        return lax.while_loop(lambda state: state[0] < rounds, more, (jnp.int32(1), y))[1]

    tok_spec = P(('data', 'expert'), None)
    w_spec = P('expert', None, None)
    return jax.shard_map(local_moe, mesh=mesh, in_specs=(tok_spec, tok_spec, tok_spec, w_spec, w_spec), out_specs=tok_spec, check_vma=False)
```
